32 devices in a mesh: grp: 2 (over x), space: 16 (over z, y, core).
Axes of the slice: x: 2, y: 2, z: 4, core: 2. Of those that a mesh axis runs over, the one named last changes fastest.
Arguments:
- propagator: bfloat16 [4, 3, 4, 12, 32768], P('grp', None, None, None, 'space'), parts along dimension 0, may hold values from -6 to 6
- eigvecs: bfloat16 [4, 3, 256, 32768], P('grp', None, None, 'space'), parts along dimension 0, may hold values from -6 to 6
- operator_weights: float32 [256, 2, 256], P('grp'), parts along dimension 0, may hold values from -0.375 to 0.375
- sink_time: int32 [2], P('grp'), parts along dimension 0, may hold values from 0 to 127
- term_index: int32 [48, 3], replicated, may hold values from 0 to 11
- term_sign: int32 [48], replicated, may hold values from 0 to 1
- solver_order: int32 [32768], P('space'), may hold values from 0 to 32767, as said below
Outputs:
- solver_source: bfloat16 [4, 3, 4, 12, 32768], P('grp', None, None, None, 'space'), parts along dimension 0
The draws below stay inside these ranges and needn't reach their ends.
There are 2 independent parts, one for each index of `grp`. The reference program is written for one: setup_inputs(seed, part) draws one part's arguments, and reference() takes and returns one part's arrays. A program takes and returns all parts, laid end to end along the dimension named above; an argument that names none is the same for every part. Nothing has to cross between parts.
Inputs may be any that keep to these rules, and one draw needn't show every extreme that they name: solver_order is a permutation of the sites; split into blocks of 2048 positions and each block into pieces of 128, piece d of block e holds only sites d * 2048 to (d + 1) * 2048 - 1.
All inputs are finite; a program needn't handle non-finite values.
Results may differ from the reference program's by a relative error of at most 0.006.
Values may be sent and summed in bfloat16 or wider, within the bound.
A program may use at most 64 MiB of HBM per device.

```python
import math
import jax
import jax.numpy as jnp
from jax import lax

NVEC = 256
NMOM = 4
NTERM = 48
EXTENT = 64
TIME_EXTENT = 128
SITES_DEV = 2048
SITES = 32768
PAIR = 128


def one_permutation(block_key):
    return jax.random.permutation(block_key, SITES_DEV)


def draw_solver_order(key, part):
    owners_count = SITES // SITES_DEV
    block_keys = jax.random.split(jax.random.fold_in(key, 17), owners_count)
    shuffled = jax.vmap(one_permutation)(block_keys).astype(jnp.int32).reshape(owners_count, owners_count, PAIR)
    owner_start = (jnp.arange(owners_count, dtype=jnp.int32) * SITES_DEV)[:, None, None]
    ordered = (shuffled + owner_start).transpose(1, 0, 2)
    return ordered.reshape(SITES)


def place_ends(values, stream_key, smallest, top_value):
    spot = [jax.random.randint(jax.random.fold_in(stream_key, axis), (), 0, length) for axis, length in enumerate(values.shape)]
    main_axis = values.shape.index(max(values.shape))
    next_to = spot[:main_axis] + [(spot[main_axis] + 1) % values.shape[main_axis]] + spot[main_axis + 1:]
    return values.at[tuple(spot)].set(smallest).at[tuple(next_to)].set(top_value)


def spiked(entries, own_key, source, target, blocks, factor):
    def block_of(dim):
        return (jnp.arange(entries.shape[dim]) // (entries.shape[dim] // blocks)).reshape((-1,) + (1,) * (entries.ndim - 1 - dim))

    near = jax.random.permutation(own_key, blocks)[block_of(target)]
    far = (block_of(target) + blocks // 2) % blocks
    return jnp.where((block_of(source) == near) | (block_of(source) == far), factor * entries, entries)


def steps_of(rng, extent, shards, smallest, top_value):
    loudness = 1.0
    for position, parts in shards:
        draws = jax.random.uniform(jax.random.fold_in(jax.random.fold_in(rng, 6), position), (parts,), jnp.float32, smallest / len(shards), top_value / len(shards))
        loudness = loudness * jnp.repeat(jnp.exp(draws), extent[position] // parts).reshape((-1,) + (1,) * (len(extent) - 1 - position))
    return loudness


def normal_values(own_key, dims, scale, bound, cuts=(), kind=jnp.bfloat16):
    result = jax.random.normal(own_key, dims, jnp.float32) * scale
    if len(cuts) > 0:
        result = steps_of(own_key, dims, cuts, -0.22, 0.18) * result
    return jnp.clip(result, min=-bound, max=bound).astype(kind)


def gaussian_with(key, dims, spread, limit, cuts, heavy, held_as=jnp.bfloat16):
    values = spread * jax.random.normal(key, dims, jnp.float32)
    if cuts:
        values = values * steps_of(key, dims, cuts, -0.22, 0.18)
    return jnp.clip(spiked(values, jax.random.fold_in(key, 3), *heavy), -limit, limit).astype(held_as)


def setup_inputs(seed: int = 0, part: int = 0) -> dict:
    splits = jax.random.split(jax.random.key(seed), 8)
    part_splits = jax.random.split(jax.random.fold_in(splits[7], part), 8)
    return {
        "propagator": normal_values(part_splits[0], (2, 3, 4, 12, SITES), 1.0, 6.0, ((4, 16),)),
        "eigvecs": gaussian_with(part_splits[1], (2, 3, NVEC, SITES), 1.0, 6.0, ((3, 16),), (3, 2, 16, 2.0)),
        "operator_weights": normal_values(part_splits[2], (TIME_EXTENT, 2, NVEC), NVEC ** -0.5, 0.375, (), jnp.float32),
        "sink_time": jax.random.randint(part_splits[3], (1,), 0, TIME_EXTENT).astype(jnp.int32),
        "term_index": place_ends(jax.random.randint(splits[4], (NTERM, 3), 0, 12), jax.random.fold_in(splits[4], 1), 0, 11).astype(jnp.int32),
        "term_sign": place_ends(jax.random.randint(splits[5], (NTERM,), 0, 2), jax.random.fold_in(splits[5], 1), 0, 1).astype(jnp.int32),
        "solver_order": draw_solver_order(jax.random.fold_in(splits[7], 71), part),
    }


MOMENTA = ((0, 0, 0), (1, 0, 0), (0, 1, 0), (0, 0, 1))
PRECISE = lax.Precision.HIGHEST

def phase_tables(offset, length):
    site_index = offset + jnp.arange(length, dtype=jnp.int32)
    coord_x = site_index % EXTENT
    coord_y = site_index // EXTENT % EXTENT
    coord_z = site_index // (EXTENT * EXTENT)
    windings = jnp.stack([(step_x * coord_x + step_y * coord_y + step_z * coord_z) % EXTENT for step_x, step_y, step_z in MOMENTA])
    angles = windings.astype(jnp.float32) * (2.0 * math.pi / EXTENT)
    return (jnp.cos(angles), jnp.sin(angles))

def phased_rows(prop_colour, cosine_table, sine_table):
    real_part = prop_colour[0].astype(jnp.float32)[None]
    imag_part = prop_colour[1].astype(jnp.float32)[None]
    cos_rows = cosine_table[:, None, None, :]
    sin_rows = sine_table[:, None, None, :]
    turned = jnp.stack([cos_rows * real_part + sin_rows * imag_part, cos_rows * imag_part - sin_rows * real_part])
    return turned.astype(jnp.bfloat16).reshape(-1, turned.shape[-1])

def project(eig_colour, phased, scale_in):
    from_real = jnp.dot(eig_colour[0], phased.T, preferred_element_type=jnp.float32).reshape(-1, 2, NMOM, 48)
    from_imag = jnp.dot(eig_colour[1], phased.T, preferred_element_type=jnp.float32).reshape(-1, 2, NMOM, 48)
    real_part = from_real[:, 0] + from_imag[:, 1]
    imag_part = from_real[:, 1] - from_imag[:, 0]
    return jnp.stack([real_part, imag_part]) * scale_in

def assemble(pieces):
    stacked = jnp.stack(pieces)
    vectors = stacked.shape[2]
    return stacked.transpose(3, 1, 2, 0, 4).reshape(NMOM, 2, vectors, 144)

def weighted_total(blocks, weights):
    real_sum = jnp.einsum('k,pkc->pc', weights[0], blocks[:, 0], precision=PRECISE) - jnp.einsum('k,pkc->pc', weights[1], blocks[:, 1], precision=PRECISE)
    imag_sum = jnp.einsum('k,pkc->pc', weights[0], blocks[:, 1], precision=PRECISE) + jnp.einsum('k,pkc->pc', weights[1], blocks[:, 0], precision=PRECISE)
    return jnp.stack([real_sum, imag_sum], axis=1)

def term_tables(term_index, term_sign):
    channels = jnp.arange(12, dtype=jnp.int32)
    first_pick = (term_index[:, 0:1] == channels[None]).astype(jnp.float32)
    second_pick = (term_index[:, 1:2] == channels[None]).astype(jnp.float32)
    sign_values = (2 * term_sign - 1).astype(jnp.float32)
    placement = (term_index[None, :, 2] == channels[:, None]).astype(jnp.float32) * sign_values[None]
    return (first_pick, second_pick, placement)

def contract(blocks, weighted, first_pick, second_pick, placement):
    vectors = blocks.shape[2]
    block_grid = blocks.reshape(NMOM, 2, vectors, 12, 12)
    first_terms = jnp.einsum('mi,pqkij->pqkmj', first_pick, block_grid, precision=PRECISE)
    second_terms = jnp.einsum('mi,pqij->pqmj', second_pick, weighted.reshape(NMOM, 2, 12, 12), precision=PRECISE)[:, :, None]
    real_part = first_terms[:, 0] * second_terms[:, 0] - first_terms[:, 1] * second_terms[:, 1]
    imag_part = first_terms[:, 0] * second_terms[:, 1] + first_terms[:, 1] * second_terms[:, 0]
    product = jnp.stack([real_part, imag_part], axis=1)
    return jnp.einsum('cm,pqkmj->pqkcj', placement, product, precision=PRECISE).reshape(NMOM, 2, vectors, 144)

def rebuild(coeffs, eig_colour, colour, cosine_table, sine_table, scale_out):
    vectors = coeffs.shape[2]
    colour_block = coeffs.reshape(NMOM, 2, vectors, 3, 48)[:, :, :, colour]
    coeff_table = colour_block.transpose(2, 1, 0, 3).reshape(vectors, 2 * NMOM * 48)
    from_real = jnp.dot(coeff_table.T, eig_colour[0], preferred_element_type=jnp.float32).reshape(2, NMOM, 48, -1)
    from_imag = jnp.dot(coeff_table.T, eig_colour[1], preferred_element_type=jnp.float32).reshape(2, NMOM, 48, -1)
    real_part = from_real[0] - from_imag[1]
    imag_part = from_real[1] + from_imag[0]
    cos_rows = cosine_table[:, None, :]
    sin_rows = sine_table[:, None, :]
    out_real = lax.optimization_barrier(jnp.sum(cos_rows * real_part - sin_rows * imag_part, axis=0))
    out_imag = lax.optimization_barrier(jnp.sum(cos_rows * imag_part + sin_rows * real_part, axis=0))
    return jnp.stack([out_real, out_imag]) * scale_out

def reference(propagator, eigvecs, operator_weights, sink_time, term_index, term_sign, solver_order):
    cosine_table, sine_table = phase_tables(0, SITES)
    scale_in = 1.0 / math.sqrt(3.0 * SITES)
    pieces = []
    for colour in range(3):
        phased = phased_rows(propagator[:, colour], cosine_table, sine_table)
        pieces.append(project(eigvecs[:, colour], phased, scale_in))
    blocks = assemble(pieces)
    weights = lax.dynamic_index_in_dim(operator_weights, sink_time[0], 0, keepdims=False)
    first_pick, second_pick, placement = term_tables(term_index, term_sign)
    weighted = weighted_total(blocks, weights)
    coeffs = contract(blocks, weighted, first_pick, second_pick, placement).astype(jnp.bfloat16)
    scale_out = 1.0 / math.sqrt(NMOM * NVEC)
    colours = [rebuild(coeffs, eigvecs[:, colour], colour, cosine_table, sine_table, scale_out) for colour in range(3)]
    source = jnp.stack(colours, axis=1).astype(jnp.bfloat16).reshape(2, 3, 4, 12, SITES)
    return jnp.take(source, solver_order, axis=4)
```

```python
import functools
import math

import jax
import jax.numpy as jnp
from jax import lax
from jax.experimental import pallas as pl
from jax.experimental.pallas import tpu as pltpu
from jax.sharding import PartitionSpec as P

NMOM = 4
EXTENT = 64
MOMENTA = ((0, 0, 0), (1, 0, 0), (0, 1, 0), (0, 0, 1))
HIGH = lax.Precision.HIGHEST
F32 = jnp.float32
BF16 = jnp.bfloat16
MESH = pl.DeviceIdType.MESH


def phase_tables(offset, length):
    site_index = offset + jnp.arange(length, dtype=jnp.int32)
    coord_x = site_index % EXTENT
    coord_y = site_index // EXTENT % EXTENT
    coord_z = site_index // (EXTENT * EXTENT)
    windings = jnp.stack(
        [
            (step_x * coord_x + step_y * coord_y + step_z * coord_z) % EXTENT
            for step_x, step_y, step_z in MOMENTA
        ]
    )
    angles = windings.astype(F32) * (2.0 * math.pi / EXTENT)
    return jnp.concatenate([jnp.cos(angles), jnp.sin(angles)])


def term_matrices(term_index, term_sign):
    row = jnp.arange(24, dtype=jnp.int32)
    channel = 4 * (row // 8) + row % 4
    imag = (row // 4) % 2
    terms = term_index.shape[0]

    def pick(which, part):
        hit = (term_index[:, which : which + 1] == channel[None]) & (imag[None] == part)
        return hit.astype(F32)

    picks = jnp.concatenate([pick(0, 0), pick(0, 1), pick(1, 0), pick(1, 1)])
    signs = (2 * term_sign - 1).astype(F32)
    place = (pick(2, 0).T * signs[None], pick(2, 1).T * signs[None])
    return picks, jnp.concatenate(place, axis=1), terms


def swap_halves(x):
    top, bottom = x[..., :4, :], x[..., 4:, :]
    return jnp.concatenate([-bottom, top], axis=-2)


def kernel(
    n, units, terms, columns, scale_in, scale_out, chunk,
    prop, eig_hbm, trig, weights, picks, place, order, out,
    eig, acc, blocks, from_core, summed, from_chips, coeffs, lhs, source, wanted, staged,
    eig_sem, core_send, core_recv, chip_send, chip_recv, all_send, all_recv,
    fwd_send, fwd_recv, index_send, index_recv, out_send, out_recv, own_sem,
):
    me = lax.axis_index("space")
    chips = n // 2
    core = lax.rem(me, 2)
    chip = me // 2
    partner = me + 1 - 2 * core
    length = eig.shape[-1]
    nvec = eig.shape[2]
    filled = NMOM * columns // (2 * units)

    def to(device):
        return {"space": device}

    loads = []
    for colour in range(3):
        load = pltpu.make_async_copy(eig_hbm.at[:, colour], eig.at[:, colour], eig_sem.at[colour])
        load.start()
        loads.append(load)

    barrier = pltpu.get_barrier_semaphore()

    def greet(t, carry):
        pl.semaphore_signal(barrier, inc=1, device_id=to(lax.rem(me + t, n)), device_id_type=MESH)
        return carry

    lax.fori_loop(1, n, greet, 0)

    if filled < chips:
        blocks[filled:] = jnp.zeros((chips - filled,) + blocks.shape[1:], F32)

    def index_copy(slot, device, sem_slot):
        return pltpu.make_async_remote_copy(
            src_ref=order.at[slot], dst_ref=wanted.at[me],
            send_sem=index_send.at[slot], recv_sem=index_recv.at[sem_slot],
            device_id=to(device), device_id_type=MESH,
        )

    for colour in range(3):
        loads[colour].wait()
        acc[...] = jnp.zeros_like(acc)

        def project(step, carry, colour=colour):
            sites = pl.ds(pl.multiple_of(step * chunk, chunk), chunk)
            real = prop[0, colour, :, :, sites].astype(F32)
            imag = prop[1, colour, :, :, sites].astype(F32)
            straight = jnp.concatenate([real, imag], axis=1)
            crossed = jnp.concatenate([imag, -real], axis=1)
            first, second = [straight], [crossed]
            for p in range(1, NMOM):
                cosine = trig[p : p + 1, sites][None]
                sine = trig[NMOM + p : NMOM + p + 1, sites][None]
                first.append(cosine * straight + sine * crossed)
                second.append(cosine * crossed - sine * straight)
            rows = NMOM * columns * 8
            first = jnp.concatenate(first).reshape(rows, chunk).astype(BF16)
            second = jnp.concatenate(second).reshape(rows, chunk).astype(BF16)
            dims = (((1,), (1,)), ((), ()))
            acc[...] += lax.dot_general(
                first, eig[0, colour, :, sites], dims, preferred_element_type=F32
            ) + lax.dot_general(
                second, eig[1, colour, :, sites], dims, preferred_element_type=F32
            )
            return carry

        lax.fori_loop(0, length // chunk, project, 0)
        blocks[:filled, :, :, colour] = (acc[...] * scale_in).reshape(filled, 2, units, 8, nvec)
        if colour == 0:
            pl.semaphore_wait(barrier, n - 1)

            def send_index(t, carry):
                peer = lax.rem(me + t, n)
                index_copy(peer, peer, me).start()
                return carry

            lax.fori_loop(1, n, send_index, 0)
            wanted[pl.ds(me, 1)] = order[pl.ds(me, 1)]

    core_copy = pltpu.make_async_remote_copy(
        src_ref=blocks.at[:, 1 - core], dst_ref=from_core,
        send_sem=core_send, recv_sem=core_recv, device_id=to(partner), device_id_type=MESH,
    )
    core_copy.start()
    core_copy.wait()

    def chip_copy(slot, device, sem_slot):
        return pltpu.make_async_remote_copy(
            src_ref=summed.at[slot], dst_ref=from_chips.at[chip],
            send_sem=chip_send.at[slot], recv_sem=chip_recv.at[sem_slot],
            device_id=to(device), device_id_type=MESH,
        )

    def send_sum(t, carry):
        other = lax.rem(chip + t, chips)
        summed[pl.ds(other, 1)] = (
            blocks[pl.ds(other, 1), pl.ds(core, 1)][:, 0] + from_core[pl.ds(other, 1)]
        ).astype(BF16)
        chip_copy(other, other * 2 + core, chip).start()
        return carry

    lax.fori_loop(1, chips, send_sum, 0)
    acc_rows = units * 24

    def add_sum(t, total):
        other = lax.rem(chip + t, chips)
        chip_in(other).wait_recv()
        return total + from_chips[pl.ds(other, 1)].astype(F32).reshape(acc_rows, nvec)

    def chip_in(other):
        return pltpu.make_async_remote_copy(
            src_ref=summed.at[other], dst_ref=from_chips.at[other],
            send_sem=chip_send.at[other], recv_sem=chip_recv.at[other],
            device_id=to(other * 2 + core), device_id_type=MESH,
        )

    own = (blocks[pl.ds(chip, 1), pl.ds(core, 1)][:, 0] + from_core[pl.ds(chip, 1)]).reshape(
        acc_rows, nvec
    )
    total = lax.fori_loop(1, chips, add_sum, own)

    weight_real, weight_imag = weights[0:1, :], weights[1:2, :]
    for unit in range(units):
        block = total[unit * 24 : (unit + 1) * 24]
        picked = lax.dot_general(
            picks[...], block, (((1,), (0,)), ((), ())), precision=HIGH, preferred_element_type=F32
        )
        first_real, first_imag = picked[:terms], picked[terms : 2 * terms]
        other_real, other_imag = picked[2 * terms : 3 * terms], picked[3 * terms :]
        second_real = jnp.sum(
            weight_real * other_real - weight_imag * other_imag, axis=1, keepdims=True
        )
        second_imag = jnp.sum(
            weight_real * other_imag + weight_imag * other_real, axis=1, keepdims=True
        )
        product = jnp.concatenate(
            [
                first_real * second_real - first_imag * second_imag,
                first_real * second_imag + first_imag * second_real,
            ]
        )
        made = lax.dot_general(
            place[...], product, (((1,), (0,)), ((), ())), precision=HIGH,
            preferred_element_type=F32,
        )
        coeffs[pl.ds(me, 1), unit] = made.reshape(1, 3, 8, nvec).astype(BF16)

    def gather_copy(slot, device, send_slot):
        return pltpu.make_async_remote_copy(
            src_ref=coeffs.at[slot], dst_ref=coeffs.at[slot],
            send_sem=all_send.at[send_slot], recv_sem=all_recv.at[slot // 2],
            device_id=to(device), device_id_type=MESH,
        )

    def forward_copy(slot):
        return pltpu.make_async_remote_copy(
            src_ref=coeffs.at[slot], dst_ref=coeffs.at[slot],
            send_sem=fwd_send.at[slot // 2], recv_sem=fwd_recv.at[slot // 2],
            device_id=to(partner), device_id_type=MESH,
        )

    def send_coeffs(t, carry):
        other = lax.rem(chip + t, chips)
        gather_copy(me, other * 2 + core, other).start()
        return carry

    lax.fori_loop(1, chips, send_coeffs, 0)
    forward_copy(me).start()

    def relay(t, carry):
        other = lax.rem(chip + chips - t, chips)
        slot = other * 2 + core
        gather_copy(slot, slot, other).wait_recv()
        forward_copy(slot).start()
        return carry

    lax.fori_loop(1, chips, relay, 0)

    def take_forwarded(c, carry):
        forward_copy(c * 2 + 1 - core).wait_recv()
        return carry

    lax.fori_loop(0, chips, take_forwarded, 0)

    for colour in range(3):
        table = coeffs[:, :, colour].astype(F32).reshape(n * units, 8, nvec)[: NMOM * columns]
        rows = NMOM * columns * 8
        lhs[0] = table.reshape(rows, nvec).astype(BF16)
        lhs[1] = swap_halves(table).reshape(rows, nvec).astype(BF16)

        def rebuild(step, carry, colour=colour):
            sites = pl.ds(pl.multiple_of(step * chunk, chunk), chunk)
            grid = jnp.dot(
                lhs[0], eig[0, colour, :, sites], preferred_element_type=F32
            ) + jnp.dot(lhs[1], eig[1, colour, :, sites], preferred_element_type=F32)
            grid = grid.reshape(NMOM, columns, 8, chunk)
            straight, crossed = grid[0], None
            for p in range(1, NMOM):
                straight = straight + trig[p : p + 1, sites][None] * grid[p]
                turned = trig[NMOM + p : NMOM + p + 1, sites][None] * grid[p]
                crossed = turned if crossed is None else crossed + turned
            made = (straight + swap_halves(crossed)) * scale_out
            source[colour * columns * 8 : (colour + 1) * columns * 8, sites] = made.reshape(
                columns * 8, chunk
            ).astype(BF16)
            return carry

        lax.fori_loop(0, length // chunk, rebuild, 0)

    def index_in(t, carry):
        other = lax.rem(me + t, n)
        pltpu.make_async_remote_copy(
            src_ref=order.at[other], dst_ref=wanted.at[other],
            send_sem=index_send.at[other], recv_sem=index_recv.at[other],
            device_id=to(other), device_id_type=MESH,
        ).wait_recv()
        return carry

    lax.fori_loop(1, n, index_in, 0)

    piece = order.shape[-1]

    def choose(peer):
        local = wanted[pl.ds(peer, 1)][0] - me * length
        site = lax.broadcasted_iota(jnp.int32, (length, piece), 0)
        onehot = jnp.where(site == local, 1.0, 0.0).astype(BF16)
        chosen = jnp.dot(source[...], onehot, preferred_element_type=F32).astype(BF16)
        staged[pl.ds(peer, 1)] = chosen[None]

    def out_copy(slot, device, dst, sem_slot):
        return pltpu.make_async_remote_copy(
            src_ref=staged.at[slot], dst_ref=out.at[dst],
            send_sem=out_send.at[slot], recv_sem=out_recv.at[sem_slot],
            device_id=to(device), device_id_type=MESH,
        )

    def send_piece(t, carry):
        peer = lax.rem(me + t, n)
        choose(peer)
        out_copy(peer, peer, me, me).start()
        return carry

    lax.fori_loop(1, n, send_piece, 0)
    choose(me)
    keep = pltpu.make_async_copy(staged.at[me], out.at[me], own_sem)
    keep.start()

    def close(t, carry):
        peer = lax.rem(me + t, n)
        index_copy(peer, peer, me).wait_send()
        out_copy(peer, peer, me, me).wait_send()
        return carry

    def close_chips(t, carry):
        other = lax.rem(chip + t, chips)
        chip_copy(other, other * 2 + core, chip).wait_send()
        gather_copy(me, other * 2 + core, other).wait_send()
        return carry

    def close_forward(c, carry):
        forward_copy(c * 2 + core).wait_send()
        return carry

    def take_piece(t, carry):
        peer = lax.rem(me + n - t, n)
        out_copy(peer, peer, peer, peer).wait_recv()
        return carry

    lax.fori_loop(1, chips, close_chips, 0)
    lax.fori_loop(0, chips, close_forward, 0)
    lax.fori_loop(1, n, close, 0)
    lax.fori_loop(1, n, take_piece, 0)
    keep.wait()


def on_device(
    propagator, eigvecs, operator_weights, sink_time, term_index, term_sign, solver_order
):
    columns, length = propagator.shape[3:]
    nvec = eigvecs.shape[2]
    n = lax.axis_size("space")
    chips = n // 2
    piece = length // n
    units = -(-NMOM * columns // n)
    trig = phase_tables(lax.axis_index("space") * length, length)
    weights = lax.dynamic_index_in_dim(operator_weights, sink_time[0], 0, keepdims=False)
    picks, place, terms = term_matrices(term_index, term_sign)
    rows = NMOM * columns * 8
    out_rows = 3 * columns * 8
    unit = (units, 3, 8, nvec)
    vmem = pl.BlockSpec(memory_space=pltpu.VMEM)
    hbm = pl.BlockSpec(memory_space=pl.ANY)
    dma = pltpu.SemaphoreType.DMA
    gathered = pl.pallas_call(
        functools.partial(
            kernel, n, units, terms, columns, 1.0 / math.sqrt(3.0 * length * n),
            1.0 / math.sqrt(NMOM * nvec), 512,
        ),
        out_shape=jax.ShapeDtypeStruct((n, out_rows, piece), BF16),
        in_specs=[vmem, hbm, vmem, vmem, vmem, vmem, vmem],
        out_specs=hbm,
        scratch_shapes=[
            pltpu.VMEM(eigvecs.shape, BF16),
            pltpu.VMEM((rows, nvec), F32),
            pltpu.VMEM((chips, 2) + unit, F32),
            pltpu.VMEM((chips,) + unit, F32),
            pltpu.VMEM((chips,) + unit, BF16),
            pltpu.VMEM((chips,) + unit, BF16),
            pltpu.VMEM((n,) + unit, BF16),
            pltpu.VMEM((2, rows, nvec), BF16),
            pltpu.VMEM((out_rows, length), BF16),
            pltpu.VMEM((n, 1, piece), jnp.int32),
            pltpu.VMEM((n, out_rows, piece), BF16),
            dma((3,)), dma, dma, dma((chips,)), dma((chips,)), dma((chips,)), dma((chips,)),
            dma((chips,)), dma((chips,)), dma((n,)), dma((n,)), dma((n,)), dma((n,)), dma,
        ],
        compiler_params=pltpu.CompilerParams(
            collective_id=0, has_side_effects=True, vmem_limit_bytes=60 * 2**20
        ),
    )(
        propagator.transpose(0, 1, 3, 2, 4), eigvecs, trig, weights, picks, place,
        solver_order.reshape(n, 1, piece),
    )
    placed = gathered.reshape(n, 3, columns, 2, 4, piece).transpose(3, 1, 4, 2, 0, 5)
    return placed.reshape(2, 3, 4, columns, length)


def solution(mesh):
    return jax.shard_map(
        on_device,
        mesh=mesh,
        in_specs=(
            P("grp", None, None, None, "space"),
            P("grp", None, None, "space"),
            P("grp", None, None),
            P("grp"),
            P(),
            P(),
            P("space"),
        ),
        out_specs=P("grp", None, None, None, "space"),
        check_vma=False,
    )
```

```python
import functools
import math

import jax
import jax.numpy as jnp
from jax import lax
from jax.experimental import pallas as pl
from jax.experimental.pallas import tpu as pltpu
from jax.sharding import PartitionSpec as P

NMOM = 4
EXTENT = 64
MOMENTA = ((0, 0, 0), (1, 0, 0), (0, 1, 0), (0, 0, 1))
HIGH = lax.Precision.HIGHEST
F32 = jnp.float32
BF16 = jnp.bfloat16
MESH = pl.DeviceIdType.MESH


def swap_halves(x):
    top, bottom = x[..., :4, :], x[..., 4:, :]
    return jnp.concatenate([-bottom, top], axis=-2)


def dot32(a, b):
    return jnp.dot(a, b, precision=HIGH, preferred_element_type=F32)


def kernel(
    n, units, columns, scale_in, scale_out, chunk,
    prop, eig_hbm, sink, table_weights, term_rows, term_sign, order, out,
    eig, trig, acc, blocks, from_core, summed, from_chips, coeffs, lhs, source, wanted, onehot,
    staged, eig_sem, core_send, core_recv, chip_send, chip_recv, all_send, all_recv,
    fwd_send, fwd_recv, index_send, index_recv, out_send, out_recv, own_sem,
):
    me = lax.axis_index("space")
    chips = n // 2
    core = lax.rem(me, 2)
    chip = me // 2
    partner = me + 1 - 2 * core
    length = eig.shape[-1]
    nvec = eig.shape[2]
    piece = order.shape[-1]
    filled = NMOM * columns // (2 * units)
    steps = length // chunk
    rows = NMOM * columns * 8

    def each(lower, upper, body):
        def step(i, carry):
            body(i)
            return carry

        lax.fori_loop(lower, upper, step, 0)

    def remote(src, dst, send_sem, recv_sem, device):
        return pltpu.make_async_remote_copy(
            src_ref=src, dst_ref=dst, send_sem=send_sem, recv_sem=recv_sem,
            device_id={"space": device}, device_id_type=MESH,
        )

    loads = []
    for colour in range(3):
        load = pltpu.make_async_copy(eig_hbm.at[:, colour], eig.at[:, colour], eig_sem.at[colour])
        load.start()
        loads.append(load)

    barrier = pltpu.get_barrier_semaphore()
    each(1, n, lambda t: pl.semaphore_signal(
        barrier, inc=1, device_id={"space": lax.rem(me + t, n)}, device_id_type=MESH
    ))

    site = me * length + lax.broadcasted_iota(jnp.int32, (1, length), 1)
    bits = EXTENT.bit_length() - 1
    low = EXTENT - 1
    coords = (site & low, (site >> bits) & low, site >> (2 * bits))
    for p in range(1, NMOM):
        winding = sum(step * coord for step, coord in zip(MOMENTA[p], coords) if step) & low
        angle = winding.astype(F32) * (2.0 * math.pi / EXTENT)
        trig[p : p + 1, :] = jnp.cos(angle)
        trig[NMOM + p : NMOM + p + 1, :] = jnp.sin(angle)
    terms = term_rows.shape[1]
    eye = lax.broadcasted_iota(jnp.int32, (terms, terms), 0) == lax.broadcasted_iota(
        jnp.int32, (terms, terms), 1
    )
    lane = lax.broadcasted_iota(jnp.int32, (terms, 24), 1)
    lane_channel = (4 * (lane >> 3) + (lane & 3)).astype(F32)
    lane_imag = (lane >> 2) & 1
    picks = []
    for which in range(2):
        row = term_rows[which : which + 1, :].astype(F32)
        column = jnp.sum(jnp.where(eye, row, 0.0), axis=1, keepdims=True)
        for part in range(2):
            hit = (lane_channel == column) & (lane_imag == part)
            picks.append(jnp.where(hit, 1.0, 0.0))
    picks = jnp.concatenate(picks)
    sub = lax.broadcasted_iota(jnp.int32, (24, terms), 0)
    target = 4 * (sub >> 3) + (sub & 3) == term_rows[2:3, :]
    signs = (2 * term_sign[...] - 1).astype(F32)
    place_real = jnp.where(target & (((sub >> 2) & 1) == 0), signs, 0.0)
    place_imag = jnp.where(target & (((sub >> 2) & 1) == 1), signs, 0.0)
    time_index = lax.broadcasted_iota(jnp.int32, table_weights.shape, 0)
    weights = jnp.sum(jnp.where(time_index == sink[0], table_weights[...], 0.0), axis=0)
    weight_real, weight_imag = weights[0:1, :], weights[1:2, :]

    if filled < chips:
        blocks[:, filled:] = jnp.zeros((3, chips - filled) + blocks.shape[2:], F32)

    def index_copy(peer, dst, sem_slot):
        return remote(
            order.at[peer], wanted.at[dst], index_send.at[peer], index_recv.at[sem_slot], peer
        )

    def core_copy(colour):
        return remote(
            blocks.at[colour, :, 1 - core], from_core.at[colour],
            core_send.at[colour], core_recv.at[colour], partner,
        )

    def chip_copy(colour, other, dst):
        return remote(
            summed.at[colour, other], from_chips.at[colour, dst],
            chip_send.at[colour, other], chip_recv.at[colour, dst], other * 2 + core,
        )

    def send_sums(colour):
        core_copy(colour).wait()

        def send(t):
            other = lax.rem(chip + t, chips)
            summed[colour, pl.ds(other, 1)] = (
                blocks[colour, pl.ds(other, 1), pl.ds(core, 1)][:, 0]
                + from_core[colour, pl.ds(other, 1)]
            ).astype(BF16)
            chip_copy(colour, other, chip).start()

        each(1, chips, send)

    for colour in range(3):
        loads[colour].wait()
        acc[...] = jnp.zeros_like(acc)

        def project(step, colour=colour):
            sites = pl.ds(pl.multiple_of(step * chunk, chunk), chunk)
            real = prop[0, colour, :, :, sites].astype(F32)
            imag = prop[1, colour, :, :, sites].astype(F32)
            straight = jnp.concatenate([real, imag], axis=1)
            crossed = jnp.concatenate([imag, -real], axis=1)
            first, second = [straight], [crossed]
            for p in range(1, NMOM):
                cosine = trig[p : p + 1, sites][None]
                sine = trig[NMOM + p : NMOM + p + 1, sites][None]
                first.append(cosine * straight + sine * crossed)
                second.append(cosine * crossed - sine * straight)
            first = jnp.concatenate(first).reshape(rows, chunk).astype(BF16)
            second = jnp.concatenate(second).reshape(rows, chunk).astype(BF16)
            dims = (((1,), (1,)), ((), ()))
            acc[...] += lax.dot_general(
                first, eig[0, colour, :, sites], dims, preferred_element_type=F32
            ) + lax.dot_general(
                second, eig[1, colour, :, sites], dims, preferred_element_type=F32
            )

        each(0, steps, project)
        blocks[colour, :filled] = (acc[...] * scale_in).reshape(filled, 2, units, 8, nvec)
        if colour == 0:
            pl.semaphore_wait(barrier, n - 1)
            core_copy(0).start()

            def send_index(t):
                peer = lax.rem(me + t, n)
                index_copy(peer, me, me).start()

            each(1, n, send_index)
            wanted[pl.ds(me, 1)] = order[pl.ds(me, 1)]
        else:
            core_copy(colour).start()
            send_sums(colour - 1)
    send_sums(2)

    def index_in(t):
        other = lax.rem(me + t, n)
        index_copy(other, other, other).wait_recv()

    each(1, n, index_in)

    def build(peer_chip):
        position = lax.broadcasted_iota(jnp.int32, (length, piece), 0)
        for half in range(2):
            local = wanted[pl.ds(peer_chip * 2 + half, 1)][0] - me * length
            onehot[pl.ds(peer_chip, 1), :, half * piece : (half + 1) * piece] = jnp.where(
                position == local, 1.0, 0.0
            ).astype(BF16)[None]

    each(0, chips, build)

    totals = []
    for colour in range(3):
        own = blocks[colour, pl.ds(chip, 1), pl.ds(core, 1)][:, 0]
        own = (own + from_core[colour, pl.ds(chip, 1)]).reshape(units * 8, nvec)

        def add_sum(t, total, colour=colour):
            other = lax.rem(chip + chips - t, chips)
            chip_copy(colour, other, other).wait_recv()
            part = from_chips[colour, pl.ds(other, 1)].astype(F32)
            return total + part.reshape(units * 8, nvec)

        totals.append(lax.fori_loop(1, chips, add_sum, own))

    for unit in range(units):
        block = jnp.concatenate([total[unit * 8 : (unit + 1) * 8] for total in totals])
        picked = dot32(picks, block)
        first_real, first_imag = picked[:terms], picked[terms : 2 * terms]
        other_real, other_imag = picked[2 * terms : 3 * terms], picked[3 * terms :]
        second_real = jnp.sum(
            weight_real * other_real - weight_imag * other_imag, axis=1, keepdims=True
        )
        second_imag = jnp.sum(
            weight_real * other_imag + weight_imag * other_real, axis=1, keepdims=True
        )
        made = dot32(place_real, first_real * second_real - first_imag * second_imag) + dot32(
            place_imag, first_real * second_imag + first_imag * second_real
        )
        made = made.reshape(3, 8, nvec).astype(BF16)
        for colour in range(3):
            coeffs[colour, pl.ds(me, 1), unit] = made[colour : colour + 1]

    def gather_copy(colour, slot, other, device):
        return remote(
            coeffs.at[colour, slot], coeffs.at[colour, slot],
            all_send.at[colour, other], all_recv.at[colour, slot // 2], device,
        )

    def forward_copy(colour, slot):
        return remote(
            coeffs.at[colour, slot], coeffs.at[colour, slot],
            fwd_send.at[colour, slot // 2], fwd_recv.at[colour, slot // 2], partner,
        )

    for colour in range(3):
        def send_coeffs(t, colour=colour):
            other = lax.rem(chip + t, chips)
            gather_copy(colour, me, other, other * 2 + core).start()

        each(1, chips, send_coeffs)
        forward_copy(colour, me).start()

    def relay(colour):
        def pass_on(t):
            other = lax.rem(chip + chips - t, chips)
            slot = other * 2 + core
            gather_copy(colour, slot, other, slot).wait_recv()
            forward_copy(colour, slot).start()

        each(1, chips, pass_on)

    def out_copy(colour, slot, device, dst, sem_slot):
        return remote(
            staged.at[slot, colour], out.at[dst, colour],
            out_send.at[colour, slot], out_recv.at[colour, sem_slot], device,
        )

    def keep(colour):
        return pltpu.make_async_copy(
            staged.at[me, colour], out.at[me, colour], own_sem.at[colour]
        )

    relay(0)
    for colour in range(3):
        each(0, chips, lambda c, colour=colour: forward_copy(colour, c * 2 + 1 - core).wait_recv())
        table = coeffs[colour].astype(F32).reshape(n * units, 8, nvec)[: NMOM * columns]
        lhs[0] = table.reshape(rows, nvec).astype(BF16)
        lhs[1] = swap_halves(table).reshape(rows, nvec).astype(BF16)

        def rebuild(step, colour=colour):
            sites = pl.ds(pl.multiple_of(step * chunk, chunk), chunk)
            grid = jnp.dot(
                lhs[0], eig[0, colour, :, sites], preferred_element_type=F32
            ) + jnp.dot(lhs[1], eig[1, colour, :, sites], preferred_element_type=F32)
            grid = grid.reshape(NMOM, columns, 8, chunk)
            straight, crossed = grid[0], None
            for p in range(1, NMOM):
                straight = straight + trig[p : p + 1, sites][None] * grid[p]
                turned = trig[NMOM + p : NMOM + p + 1, sites][None] * grid[p]
                crossed = turned if crossed is None else crossed + turned
            made = (straight + swap_halves(crossed)) * scale_out
            source[:, sites] = made.reshape(columns * 8, chunk).astype(BF16)

        each(0, steps, rebuild)
        if colour < 2:
            relay(colour + 1)

        def choose(peer_chip, colour=colour):
            chosen = jnp.dot(
                source[...], onehot[pl.ds(peer_chip, 1)][0], preferred_element_type=F32
            ).astype(BF16)
            for half in range(2):
                staged[pl.ds(peer_chip * 2 + half, 1), colour] = chosen[
                    :, half * piece : (half + 1) * piece
                ][None]

        def send_pieces(t, colour=colour):
            other = lax.rem(chip + t, chips)
            choose(other)
            for half in range(2):
                peer = other * 2 + half
                out_copy(colour, peer, peer, me, me).start()

        each(1, chips, send_pieces)
        choose(chip)
        out_copy(colour, partner, partner, me, me).start()
        keep(colour).start()

    def close_index(t):
        peer = lax.rem(me + t, n)
        index_copy(peer, me, me).wait_send()

    each(1, n, close_index)
    for colour in range(3):
        def close(t, colour=colour):
            peer = lax.rem(me + t, n)
            out_copy(colour, peer, peer, me, me).wait_send()

        def close_chips(t, colour=colour):
            other = lax.rem(chip + t, chips)
            chip_copy(colour, other, chip).wait_send()
            gather_copy(colour, me, other, other * 2 + core).wait_send()

        def take_piece(t, colour=colour):
            peer = lax.rem(me + n - t, n)
            out_copy(colour, peer, peer, peer, peer).wait_recv()

        each(1, chips, close_chips)
        each(0, chips, lambda c, colour=colour: forward_copy(colour, c * 2 + core).wait_send())
        each(1, n, close)
        each(1, n, take_piece)
        keep(colour).wait()


def on_device(
    propagator, eigvecs, operator_weights, sink_time, term_index, term_sign, solver_order
):
    columns, length = propagator.shape[3:]
    nvec = eigvecs.shape[2]
    n = lax.axis_size("space")
    chips = n // 2
    piece = length // n
    units = -(-NMOM * columns // n)
    rows = NMOM * columns * 8
    site_rows = columns * 8
    unit = (units, 8, nvec)
    vmem = pl.BlockSpec(memory_space=pltpu.VMEM)
    smem = pl.BlockSpec(memory_space=pltpu.SMEM)
    hbm = pl.BlockSpec(memory_space=pl.ANY)
    dma = pltpu.SemaphoreType.DMA
    gathered = pl.pallas_call(
        functools.partial(
            kernel, n, units, columns, 1.0 / math.sqrt(3.0 * length * n),
            1.0 / math.sqrt(NMOM * nvec), 512,
        ),
        out_shape=jax.ShapeDtypeStruct((n, 3, site_rows, piece), BF16),
        in_specs=[vmem, hbm, smem, vmem, vmem, vmem, vmem],
        out_specs=hbm,
        scratch_shapes=[
            pltpu.VMEM(eigvecs.shape, BF16),
            pltpu.VMEM((2 * NMOM, length), F32),
            pltpu.VMEM((rows, nvec), F32),
            pltpu.VMEM((3, chips, 2) + unit, F32),
            pltpu.VMEM((3, chips) + unit, F32),
            pltpu.VMEM((3, chips) + unit, BF16),
            pltpu.VMEM((3, chips) + unit, BF16),
            pltpu.VMEM((3, n) + unit, BF16),
            pltpu.VMEM((2, rows, nvec), BF16),
            pltpu.VMEM((site_rows, length), BF16),
            pltpu.VMEM((n, 1, piece), jnp.int32),
            pltpu.VMEM((chips, length, 2 * piece), BF16),
            pltpu.VMEM((n, 3, site_rows, piece), BF16),
            dma((3,)), dma((3,)), dma((3,)), dma((3, chips)), dma((3, chips)), dma((3, chips)),
            dma((3, chips)), dma((3, chips)), dma((3, chips)), dma((n,)), dma((n,)),
            dma((3, n)), dma((3, n)), dma((3,)),
        ],
        compiler_params=pltpu.CompilerParams(
            collective_id=0, has_side_effects=True, vmem_limit_bytes=60 * 2**20
        ),
    )(
        propagator.transpose(0, 1, 3, 2, 4), eigvecs, sink_time, operator_weights,
        term_index.T, term_sign.reshape(1, -1), solver_order.reshape(n, 1, piece),
    )
    placed = gathered.reshape(n, 3, columns, 2, 4, piece).transpose(3, 1, 4, 2, 0, 5)
    return placed.reshape(2, 3, 4, columns, length)


def solution(mesh):
    return jax.shard_map(
        on_device,
        mesh=mesh,
        in_specs=(
            P("grp", None, None, None, "space"),
            P("grp", None, None, "space"),
            P("grp", None, None),
            P("grp"),
            P(),
            P(),
            P("space"),
        ),
        out_specs=P("grp", None, None, None, "space"),
        check_vma=False,
    )
```
